256 devices in a mesh: dp: 256 (over y, x, z, core).
Axes of the slice: x: 4, y: 4, z: 8, core: 2. Of those that a mesh axis runs over, the one named last changes fastest.
Arguments:
- grads: bfloat16 [256, 4096, 128], P('dp'), may hold values from -3200 to 3200
- master: float32 [4096, 128], P('dp'), may hold values from -6 to 6
- first_q: bfloat16 [4096, 128], P('dp'), may hold values from -1 to 1
- first_scale: float32 [4096], P('dp'), may hold values from 0.005 to 0.05
- second_q: bfloat16 [4096, 128], P('dp'), may hold values from 0.099609375 to 1
- second_scale: float32 [4096], P('dp'), may hold values from 2e-05 to 0.0002
Outputs:
- weights: bfloat16 [4096, 128], replicated
- master_new: float32 [4096, 128], P('dp')
- first_q_new: bfloat16 [4096, 128], P('dp')
- first_scale_new: float32 [4096], P('dp')
- second_q_new: bfloat16 [4096, 128], P('dp')
- second_scale_new: float32 [4096], P('dp')
The draws below stay inside these ranges and needn't reach their ends.
All inputs are finite; a program needn't handle non-finite values. Where the reference program divides by a largest or mean magnitude, that divisor is 1e-20 or more.
Results may differ from the reference program's by a relative error of at most 0.001.
Values may be sent and summed in bfloat16 or wider, within the bound.
No kernel may reach another device: no remote copies, remote signals or barrier semaphores. Data moves between devices by JAX's collectives and lax.ppermute only.
A program may use at most 64 MiB of HBM per device.

```python
import math
import jax
import jax.numpy as jnp
from jax import lax

D = 6144
BLK_DEV = 16
BLOCKS = 4096
N_DP = 256


def draw_grads(key, part):
    keys = jax.random.split(jax.random.fold_in(key, 17), 4)
    lane_groups = D // 128
    block_ids = jnp.arange(BLOCKS)
    row_ids = block_ids // lane_groups
    row_count = (BLOCKS + lane_groups - 1) // lane_groups
    row_scale = 10.0 ** (row_ids.astype(jnp.float32) / max(row_count - 1, 1))
    column_scale = 10.0 ** jax.random.uniform(keys[0], (lane_groups, 128), jnp.float32)
    block_cols = column_scale[block_ids % lane_groups]
    replica_scale = 2.0 ** jax.random.uniform(keys[1], (N_DP,), jnp.float32, -1.0, 1.0)
    owners = jax.random.permutation(keys[2], N_DP)
    spike = jnp.where((block_ids // BLK_DEV)[None, :] == owners[:, None], 4.0, 1.0)
    noise = jnp.clip(jax.random.normal(keys[3], (N_DP, BLOCKS, 128), jnp.float32), -4.0, 4.0)
    values = noise * row_scale[None, :, None] * block_cols[None] * replica_scale[:, None, None] * spike[:, :, None]
    return values.astype(jnp.bfloat16)


def block_scale(stream_key, shape, pieces, least, largest):
    loudness = 1.0
    for dim, parts in pieces:
        heights = jax.random.uniform(jax.random.fold_in(jax.random.fold_in(stream_key, 6), dim), (parts,), jnp.float32, least / len(pieces), largest / len(pieces))
        loudness = loudness * jnp.repeat(jnp.exp(heights), shape[dim] // parts).reshape((-1,) + (1,) * (len(shape) - 1 - dim))
    return loudness


def gaussian(rng, dims, deviation, reach, pieces=(), dtype=jnp.bfloat16):
    array = jax.random.normal(rng, dims, jnp.float32) * deviation
    if len(pieces) > 0:
        array = block_scale(rng, dims, pieces, -0.22, 0.18) * array
    return jnp.clip(array, min=-reach, max=reach).astype(dtype)


def setup_inputs(seed: int = 0) -> dict:
    key_list = jax.random.split(jax.random.key(seed), 7)
    return {
        "grads": draw_grads(jax.random.fold_in(key_list[6], 71), 0),
        "master": gaussian(key_list[1], (BLOCKS, 128), 1.0, 6.0, ((0, 256),), jnp.float32),
        "first_q": jnp.clip(jax.random.uniform(key_list[2], (BLOCKS, 128), jnp.float32, -1.0, 1.0) * block_scale(key_list[2], (BLOCKS, 128), ((0, 256),), -0.4, 0.0), -1.0, 1.0).astype(jnp.bfloat16),
        "first_scale": jnp.clip(jnp.exp(math.log(0.05) - 2.3025851 * jax.random.uniform(key_list[3], (BLOCKS,), jnp.float32) ** block_scale(key_list[3], (BLOCKS,), ((0, 256),), -0.2, 0.2)), 0.005, 0.05),
        "second_q": jnp.clip(0.099609375 + 0.9003906 * jax.random.uniform(key_list[4], (BLOCKS, 128), jnp.float32) ** block_scale(key_list[4], (BLOCKS, 128), ((0, 256),), -0.2, 0.2), 0.099609375, 1.0).astype(jnp.bfloat16),
        "second_scale": jnp.clip(jnp.exp(math.log(0.0002) - 2.3025851 * jax.random.uniform(key_list[5], (BLOCKS,), jnp.float32) ** block_scale(key_list[5], (BLOCKS,), ((0, 256),), -0.2, 0.2)), 1.9999999494757503e-05, 0.0002),
    }


beta_one = 0.9
beta_two = 0.95
learn_rate = 0.05
decay_rate = 0.1
adam_epsilon = 1e-08
clip_rms = 0.01
first_fix = 1.0 - 0.9 ** 10
second_fix = 1.0 - 0.95 ** 10

def reference(grads, master, first_q, first_scale, second_q, second_scale):

    def accumulate(carry, piece):
        return (carry + piece.astype(jnp.float32), None)
    start = jnp.zeros(grads.shape[1:], jnp.float32)
    total, _ = lax.scan(accumulate, start, grads)
    norm = jnp.sqrt(jnp.sum(total * total))
    limit = clip_rms * jnp.sqrt(jnp.float32(total.shape[0] * total.shape[1]))
    factor = jnp.minimum(1.0, limit / (norm + 1e-06))
    clipped = factor * total
    first = first_q.astype(jnp.float32) * first_scale[:, None]
    second = second_q.astype(jnp.float32) * second_scale[:, None]
    first_new = beta_one * first + (1.0 - beta_one) * clipped
    second_new = beta_two * second + (1.0 - beta_two) * clipped * clipped
    change = first_new / first_fix / (jnp.sqrt(second_new / second_fix) + adam_epsilon)
    master_new = master * (1.0 - learn_rate * decay_rate) - learn_rate * change
    first_scale_new = lax.optimization_barrier(jnp.max(jnp.abs(first_new), axis=1)) + 1e-08
    second_scale_new = lax.optimization_barrier(jnp.max(jnp.abs(second_new), axis=1)) + 1e-08
    first_q_new = (first_new / first_scale_new[:, None]).astype(jnp.bfloat16)
    second_q_new = (second_new / second_scale_new[:, None]).astype(jnp.bfloat16)
    weights = master_new.astype(jnp.bfloat16)
    return (weights, master_new, first_q_new, first_scale_new, second_q_new, second_scale_new)
```

```python
import jax
import jax.numpy as jnp
from jax import lax
from jax.sharding import Mesh
from jax.sharding import PartitionSpec as P

DP = ("y", "x", "z", "c")


beta_one = 0.9
beta_two = 0.95
learn_rate = 0.05
decay_rate = 0.1
adam_epsilon = 1e-08
clip_rms = 0.01
first_fix = 1.0 - 0.9**10
second_fix = 1.0 - 0.95**10


def exchange(x, axes):
    return lax.all_to_all(x, axes, split_axis=0, concat_axis=0, tiled=True)


def sent_to_all(x, axes):
    return exchange(jnp.broadcast_to(x, (lax.axis_size(axes), *x.shape)), axes)


def advance(clipped, master, first, second):
    first_new = beta_one * first + (1.0 - beta_one) * clipped
    second_new = beta_two * second + (1.0 - beta_two) * clipped * clipped
    change = first_new / first_fix / (jnp.sqrt(second_new / second_fix) + adam_epsilon)
    master_new = master * (1.0 - learn_rate * decay_rate) - learn_rate * change
    return master_new, first_new, second_new


def shards(grads, master, first_q, first_scale, second_q, second_scale):
    blocks, width = grads.shape[1:]
    rows = master.shape[0]
    planes, line, cores = lax.axis_size(("y", "x")), lax.axis_size("z"), lax.axis_size("c")
    held = line * rows
    first = first_q.astype(jnp.float32) * first_scale[:, None]
    second = second_q.astype(jnp.float32) * second_scale[:, None]

    local = grads[0].reshape(planes, line, cores, rows, width).swapaxes(1, 2)
    arrived = exchange(local.reshape(planes * cores, held, width), ("y", "x", "c"))
    part = arrived.astype(jnp.float32).sum(axis=0)

    packed = jnp.concatenate([part, master, first, second], axis=0)
    shared = sent_to_all(packed, "z")
    total = shared[:, :held].sum(axis=0)
    states = shared[:, held:].reshape(line, 3, rows, width)
    line_master, line_first, line_second = (
        states[:, i].reshape(held, width) for i in range(3)
    )

    squares = sent_to_all(jnp.sum(total * total, axis=0, keepdims=True), ("y", "x", "c")).sum()
    limit = clip_rms * jnp.sqrt(jnp.float32(blocks * width))
    factor = jnp.minimum(1.0, limit / (jnp.sqrt(squares) + 1e-06))

    line_new, _, _ = advance(factor * total, line_master, line_first, line_second)
    weights = sent_to_all(line_new.astype(jnp.bfloat16), ("y", "x"))
    weights = weights.reshape(planes, line, 1, rows, width)
    partner = lax.ppermute(weights, "c", [(0, 1), (1, 0)])
    mine = jnp.arange(cores) == lax.axis_index("c")
    weights = jnp.where(mine[:, None, None], weights, partner).reshape(blocks, width)

    own = lax.dynamic_slice_in_dim(total, lax.axis_index("z") * rows, rows, 0)
    master_new, first_new, second_new = advance(factor * own, master, first, second)
    first_scale_new = jnp.max(jnp.abs(first_new), axis=1) + 1e-08
    second_scale_new = jnp.max(jnp.abs(second_new), axis=1) + 1e-08
    first_q_new = (first_new / first_scale_new[:, None]).astype(jnp.bfloat16)
    second_q_new = (second_new / second_scale_new[:, None]).astype(jnp.bfloat16)
    return (weights, master_new, first_q_new, first_scale_new, second_q_new, second_scale_new)


def solution(mesh):
    torus = Mesh(mesh.devices.reshape(4, 4, 8, 2), DP)
    in_specs = (P(DP, None, None), P(DP, None), P(DP, None), P(DP), P(DP, None), P(DP))
    out_specs = (P(), P(DP, None), P(DP, None), P(DP), P(DP, None), P(DP))
    return jax.shard_map(
        shards, mesh=torus, in_specs=in_specs, out_specs=out_specs, check_vma=False
    )
```

```python
import jax
import jax.numpy as jnp
from jax import lax
from jax.sharding import Mesh
from jax.sharding import PartitionSpec as P

DP = ("y", "x", "z", "c")


beta_one = 0.9
beta_two = 0.95
learn_rate = 0.05
decay_rate = 0.1
adam_epsilon = 1e-08
clip_rms = 0.01
first_fix = 1.0 - 0.9**10
second_fix = 1.0 - 0.95**10


def exchange(x, axes):
    return lax.all_to_all(x, axes, split_axis=0, concat_axis=0, tiled=True)


def sent_to_all(x, axes):
    return exchange(jnp.broadcast_to(x, (lax.axis_size(axes), *x.shape)), axes)


def doubled(x, axis):
    count = lax.axis_size(axis)
    index = lax.axis_index(axis)
    for level in range(count.bit_length() - 1):
        other = lax.ppermute(x, axis, [(i, i ^ 1 << level) for i in range(count)])
        mine = jnp.arange(2) == (index >> level & 1)
        x = jnp.where(mine[:, None, None, None, None], x, other).reshape(-1, *x.shape[1:])
    return x


def advance(clipped, master, first, second):
    first_new = beta_one * first + (1.0 - beta_one) * clipped
    second_new = beta_two * second + (1.0 - beta_two) * clipped * clipped
    change = first_new / first_fix / (jnp.sqrt(second_new / second_fix) + adam_epsilon)
    master_new = master * (1.0 - learn_rate * decay_rate) - learn_rate * change
    return master_new, first_new, second_new


def shards(grads, master, first_q, first_scale, second_q, second_scale):
    blocks, width = grads.shape[1:]
    rows = master.shape[0]
    planes, line, cores = lax.axis_size(("y", "x")), lax.axis_size("z"), lax.axis_size("c")
    held = line * rows
    swap = [(0, 1), (1, 0)]
    first = first_q.astype(jnp.float32) * first_scale[:, None]
    second = second_q.astype(jnp.float32) * second_scale[:, None]

    arrived = exchange(grads[0].reshape(planes, line * cores * rows, width), ("y", "x"))
    states = doubled(jnp.stack([master, first, second])[None], "z")
    arrived, states = lax.optimization_barrier((arrived, states))
    both = arrived.astype(jnp.float32).sum(axis=0).reshape(line, cores, rows, width)
    core = lax.axis_index("c")
    kept, sent = (lax.dynamic_index_in_dim(both, i, 1, False) for i in (core, 1 - core))
    part = (kept + lax.ppermute(sent, "c", swap)).reshape(held, width)

    total = sent_to_all(part, "z").sum(axis=0)
    line_master, line_first, line_second = (
        states[:, i].reshape(held, width) for i in range(3)
    )

    squares = sent_to_all(jnp.sum(total * total, axis=0, keepdims=True), ("y", "x", "c")).sum()
    limit = clip_rms * jnp.sqrt(jnp.float32(blocks * width))
    factor = jnp.minimum(1.0, limit / (jnp.sqrt(squares) + 1e-06))

    line_new, _, _ = advance(factor * total, line_master, line_first, line_second)
    weights = sent_to_all(line_new.astype(jnp.bfloat16), ("y", "x"))
    weights = weights.reshape(planes, line, 1, rows, width)
    partner = lax.ppermute(weights, "c", swap)
    mine = jnp.arange(cores) == lax.axis_index("c")
    weights = jnp.where(mine[:, None, None], weights, partner).reshape(blocks, width)

    own = lax.dynamic_slice_in_dim(total, lax.axis_index("z") * rows, rows, 0)
    master_new, first_new, second_new = advance(factor * own, master, first, second)
    first_scale_new = jnp.max(jnp.abs(first_new), axis=1) + 1e-08
    second_scale_new = jnp.max(jnp.abs(second_new), axis=1) + 1e-08
    first_q_new = (first_new / first_scale_new[:, None]).astype(jnp.bfloat16)
    second_q_new = (second_new / second_scale_new[:, None]).astype(jnp.bfloat16)
    return (weights, master_new, first_q_new, first_scale_new, second_q_new, second_scale_new)


def solution(mesh):
    torus = Mesh(mesh.devices.reshape(4, 4, 8, 2), DP)
    in_specs = (P(DP, None, None), P(DP, None), P(DP, None), P(DP), P(DP, None), P(DP))
    out_specs = (P(), P(DP, None), P(DP, None), P(DP), P(DP, None), P(DP))
    return jax.shard_map(
        shards, mesh=torus, in_specs=in_specs, out_specs=out_specs, check_vma=False
    )
```

```python
import jax
import jax.numpy as jnp
from jax import lax
from jax.sharding import Mesh
from jax.sharding import PartitionSpec as P

DP = ("y", "x", "z", "c")


beta_one = 0.9
beta_two = 0.95
learn_rate = 0.05
decay_rate = 0.1
adam_epsilon = 1e-08
clip_rms = 0.01
first_fix = 1.0 - 0.9**10
second_fix = 1.0 - 0.95**10


def exchange(x, axes):
    return lax.all_to_all(x, axes, split_axis=0, concat_axis=0, tiled=True)


def sent_to_all(x, axes):
    return exchange(jnp.broadcast_to(x, (lax.axis_size(axes), *x.shape)), axes)


def from_partner(x, axis, flip):
    return lax.ppermute(x, axis, [(i, i ^ flip) for i in range(lax.axis_size(axis))])


def flips(axis):
    levels = lax.axis_size(axis).bit_length() - 1
    return [(3 << level - 1 if level > 1 else 1 << level, level) for level in range(levels)]


def summed(x, axis):
    for flip, _ in flips(axis):
        x = x + from_partner(x, axis, flip)
    return x


def gathered(x, axis):
    x = x[None]
    place = lax.axis_index(axis)[None]
    for flip, level in reversed(flips(axis)):
        other = from_partner(x, axis, flip)
        mine = jnp.arange(2) == (place[:, None] >> level & 1)
        place = jnp.where(mine, place[:, None], place[:, None] ^ flip).reshape(-1)
        x = jnp.where(mine[:, :, None, None, None], x[:, None], other[:, None]).reshape(-1, *x.shape[1:])
    return x


def advance(clipped, master, first, second):
    first_new = beta_one * first + (1.0 - beta_one) * clipped
    second_new = beta_two * second + (1.0 - beta_two) * clipped * clipped
    change = first_new / first_fix / (jnp.sqrt(second_new / second_fix) + adam_epsilon)
    master_new = master * (1.0 - learn_rate * decay_rate) - learn_rate * change
    return master_new, first_new, second_new


def shards(grads, master, first_q, first_scale, second_q, second_scale):
    blocks, width = grads.shape[1:]
    rows = master.shape[0]
    planes, line, cores = lax.axis_size(("y", "x")), lax.axis_size("z"), lax.axis_size("c")
    held = line * rows
    first = first_q.astype(jnp.float32) * first_scale[:, None]
    second = second_q.astype(jnp.float32) * second_scale[:, None]

    arrived = exchange(grads[0].reshape(planes, line * cores * rows, width), ("y", "x"))
    states = gathered(jnp.stack([master, first, second]), "z")
    arrived, states = lax.optimization_barrier((arrived, states))
    both = arrived.astype(jnp.float32).sum(axis=0).reshape(line, cores, rows, width)
    core = lax.axis_index("c")
    kept, sent = (lax.dynamic_index_in_dim(both, i, 1, False) for i in (core, 1 - core))
    part = (kept + from_partner(sent, "c", 1)).reshape(held, width)

    total = summed(part, "z")
    line_master, line_first, line_second = (
        states[:, i].reshape(held, width) for i in range(3)
    )

    squares = sent_to_all(jnp.sum(total * total, axis=0, keepdims=True), ("y", "x", "c")).sum()
    limit = clip_rms * jnp.sqrt(jnp.float32(blocks * width))
    factor = jnp.minimum(1.0, limit / (jnp.sqrt(squares) + 1e-06))

    line_new, _, _ = advance(factor * total, line_master, line_first, line_second)
    weights = sent_to_all(line_new.astype(jnp.bfloat16), ("y", "x"))
    weights = weights.reshape(planes, line, 1, rows, width)
    partner = from_partner(weights, "c", 1)
    mine = jnp.arange(cores) == lax.axis_index("c")
    weights = jnp.where(mine[:, None, None], weights, partner).reshape(blocks, width)

    own = lax.dynamic_slice_in_dim(total, lax.axis_index("z") * rows, rows, 0)
    master_new, first_new, second_new = advance(factor * own, master, first, second)
    first_scale_new = jnp.max(jnp.abs(first_new), axis=1) + 1e-08
    second_scale_new = jnp.max(jnp.abs(second_new), axis=1) + 1e-08
    first_q_new = (first_new / first_scale_new[:, None]).astype(jnp.bfloat16)
    second_q_new = (second_new / second_scale_new[:, None]).astype(jnp.bfloat16)
    return (weights, master_new, first_q_new, first_scale_new, second_q_new, second_scale_new)


def solution(mesh):
    torus = Mesh(mesh.devices.reshape(4, 4, 8, 2), DP)
    in_specs = (P(DP, None, None), P(DP, None), P(DP, None), P(DP), P(DP, None), P(DP))
    out_specs = (P(), P(DP, None), P(DP, None), P(DP), P(DP, None), P(DP))
    return jax.shard_map(
        shards, mesh=torus, in_specs=in_specs, out_specs=out_specs, check_vma=False
    )
```

```python
import jax
import jax.numpy as jnp
from jax import lax
from jax.sharding import Mesh
from jax.sharding import PartitionSpec as P

DP = ("y", "x", "z", "c")


beta_one = 0.9
beta_two = 0.95
learn_rate = 0.05
decay_rate = 0.1
adam_epsilon = 1e-08
clip_rms = 0.01
first_fix = 1.0 - 0.9**10
second_fix = 1.0 - 0.95**10


def exchange(x, axes):
    return lax.all_to_all(x, axes, split_axis=0, concat_axis=0, tiled=True)


def sent_to_all(x, axes):
    return exchange(jnp.broadcast_to(x, (lax.axis_size(axes), *x.shape)), axes)


def swapped(x):
    return lax.ppermute(x, "c", [(0, 1), (1, 0)])


def from_partner(x, flip):
    line = lax.axis_size("z")
    route = [(2 * z + c, 2 * (z ^ flip) + 1 - c) for z in range(line) for c in range(2)]
    return lax.ppermute(x, ("z", "c"), route)


FLIPS = ((1, 0), (2, 1), (6, 2))


def summed(x):
    for flip, _ in FLIPS:
        x = x + from_partner(x, flip)
    return x


def doubled(x, place, step):
    flip, level = step
    other = from_partner(x, flip)
    mine = jnp.arange(2) == (place[:, None] >> level & 1)
    place = jnp.where(mine, place[:, None], place[:, None] ^ flip).reshape(-1)
    x = jnp.where(mine[:, :, None, None, None], x[:, None], other[:, None])
    return x.reshape(-1, *x.shape[2:]), place


def advance(clipped, master, first, second):
    first_new = beta_one * first + (1.0 - beta_one) * clipped
    second_new = beta_two * second + (1.0 - beta_two) * clipped * clipped
    change = first_new / first_fix / (jnp.sqrt(second_new / second_fix) + adam_epsilon)
    master_new = master * (1.0 - learn_rate * decay_rate) - learn_rate * change
    return master_new, first_new, second_new


def shards(grads, master, first_q, first_scale, second_q, second_scale):
    blocks, width = grads.shape[1:]
    rows = master.shape[0]
    planes, line, cores = lax.axis_size(("y", "x")), lax.axis_size("z"), lax.axis_size("c")
    held = line * rows
    first = first_q.astype(jnp.float32) * first_scale[:, None]
    second = second_q.astype(jnp.float32) * second_scale[:, None]

    z, core = lax.axis_index("z"), lax.axis_index("c")
    odd = (z ^ z >> 1) & 1
    here = core ^ odd

    arrived = exchange(grads[0].reshape(planes, line * cores * rows, width), ("y", "x"))
    states = jnp.stack([master, first, second])
    states = jnp.where(odd == 1, swapped(states), states)[None]
    place = z[None]
    for step in FLIPS[:0:-1]:
        states, place = doubled(states, place, step)
    arrived, states = lax.optimization_barrier((arrived, states))
    both = arrived.astype(jnp.float32).sum(axis=0).reshape(line, cores, rows, width)
    kept, sent = (lax.dynamic_index_in_dim(both, i, 1, False) for i in (here, 1 - here))
    part = (kept + swapped(sent)).reshape(held, width)

    total = summed(part)
    total, states = lax.optimization_barrier((total, states))
    norms = sent_to_all(jnp.sum(total * total, axis=0, keepdims=True), ("y", "x", "c"))
    norms = norms.reshape(planes, cores, width)
    norms = norms[:, 0] + norms[:, 1]
    states, _ = doubled(states, place, FLIPS[0])
    line_master, line_first, line_second = (
        states[:, i].reshape(held, width) for i in range(3)
    )
    limit = clip_rms * jnp.sqrt(jnp.float32(blocks * width))
    factor = jnp.minimum(1.0, limit / (jnp.sqrt(norms.sum()) + 1e-06))

    line_new, _, _ = advance(factor * total, line_master, line_first, line_second)
    weights = sent_to_all(line_new.astype(jnp.bfloat16), ("y", "x"))
    weights = weights.reshape(planes, line, 1, rows, width)
    mine = jnp.arange(cores) == here
    weights = jnp.where(mine[:, None, None], weights, swapped(weights)).reshape(blocks, width)

    own = lax.dynamic_slice_in_dim(total, z * rows, rows, 0)
    own = jnp.where(odd == 1, swapped(own), own)
    master_new, first_new, second_new = advance(factor * own, master, first, second)
    first_scale_new = jnp.max(jnp.abs(first_new), axis=1) + 1e-08
    second_scale_new = jnp.max(jnp.abs(second_new), axis=1) + 1e-08
    first_q_new = (first_new / first_scale_new[:, None]).astype(jnp.bfloat16)
    second_q_new = (second_new / second_scale_new[:, None]).astype(jnp.bfloat16)
    return (weights, master_new, first_q_new, first_scale_new, second_q_new, second_scale_new)


def solution(mesh):
    torus = Mesh(mesh.devices.reshape(4, 4, 8, 2), DP)
    in_specs = (P(DP, None, None), P(DP, None), P(DP, None), P(DP), P(DP, None), P(DP))
    out_specs = (P(), P(DP, None), P(DP, None), P(DP), P(DP, None), P(DP))
    return jax.shard_map(
        shards, mesh=torus, in_specs=in_specs, out_specs=out_specs, check_vma=False
    )
```

```python
import functools
import math

import jax
import jax.numpy as jnp
from jax import lax
from jax.experimental import pallas as pl
from jax.experimental.pallas import tpu as pltpu
from jax.sharding import Mesh
from jax.sharding import PartitionSpec as P

DP = ("y", "x", "z", "c")


beta_one = 0.9
beta_two = 0.95
learn_rate = 0.05
decay_rate = 0.1
adam_epsilon = 1e-08
clip_rms = 0.01
first_fix = 1.0 - 0.9**10
second_fix = 1.0 - 0.95**10


def exchange(x, axes):
    return lax.all_to_all(x, axes, split_axis=0, concat_axis=0, tiled=True)


def sent_to_all(x, axes):
    return exchange(jnp.broadcast_to(x, (lax.axis_size(axes), *x.shape)), axes)


def swapped(x):
    return lax.ppermute(x, "c", [(0, 1), (1, 0)])


def from_partner(x, flip):
    line = lax.axis_size("z")
    route = [(2 * z + c, 2 * (z ^ flip) + 1 - c) for z in range(line) for c in range(2)]
    return lax.ppermute(x, ("z", "c"), route)


FLIPS = ((1, 0), (2, 1), (6, 2))


def summed(x):
    for flip, _ in FLIPS:
        x = x + from_partner(x, flip)
    return x


def doubled(x, place, step):
    flip, level = step
    other = from_partner(x, flip)
    mine = jnp.arange(2) == (place[:, None] >> level & 1)
    place = jnp.where(mine, place[:, None], place[:, None] ^ flip).reshape(-1)
    x = jnp.where(mine[:, :, None, None, None], x[:, None], other[:, None])
    return x.reshape(-1, *x.shape[2:]), place


def advance(clipped, master, first, second):
    first_new = beta_one * first + (1.0 - beta_one) * clipped
    second_new = beta_two * second + (1.0 - beta_two) * clipped * clipped
    change = first_new / first_fix / (jnp.sqrt(second_new / second_fix) + adam_epsilon)
    master_new = master * (1.0 - learn_rate * decay_rate) - learn_rate * change
    return master_new, first_new, second_new


def clip_and_advance(limit, norms, total, states, weights, factors):
    pairs = norms[...]
    squares = jnp.sum(pairs[:, 0] + pairs[:, 1], keepdims=True)
    factor = jnp.minimum(1.0, limit / (jnp.sqrt(squares) + 1e-06))
    factors[...] = jnp.broadcast_to(factor, factors.shape)
    line, _, rows, width = states.shape
    for z in range(line):
        place = pl.ds(z * rows, rows)
        new, _, _ = advance(factor * total[place], states[z, 0], states[z, 1], states[z, 2])
        new = new.astype(weights.dtype)
        for plane in range(weights.shape[0]):
            weights[plane, place] = new


def shards(grads, master, first_q, first_scale, second_q, second_scale):
    blocks, width = grads.shape[1:]
    rows = master.shape[0]
    planes, line, cores = lax.axis_size(("y", "x")), lax.axis_size("z"), lax.axis_size("c")
    held = line * rows
    first = first_q.astype(jnp.float32) * first_scale[:, None]
    second = second_q.astype(jnp.float32) * second_scale[:, None]

    z, core = lax.axis_index("z"), lax.axis_index("c")
    odd = (z ^ z >> 1) & 1
    here = core ^ odd

    arrived = exchange(grads[0].reshape(planes, line * cores * rows, width), ("y", "x"))
    states = jnp.stack([master, first, second])
    states = jnp.where(odd == 1, swapped(states), states)[None]
    place = z[None]
    for step in FLIPS[:0:-1]:
        states, place = doubled(states, place, step)
    arrived, states = lax.optimization_barrier((arrived, states))
    both = arrived.astype(jnp.float32).sum(axis=0).reshape(line, cores, rows, width)
    kept, sent = (lax.dynamic_index_in_dim(both, i, 1, False) for i in (here, 1 - here))
    part = (kept + swapped(sent)).reshape(held, width)

    total = summed(part)
    total, states = lax.optimization_barrier((total, states))
    norms = sent_to_all(jnp.sum(total * total, axis=0, keepdims=True), ("y", "x", "c"))
    states, _ = doubled(states, place, FLIPS[0])
    own = lax.dynamic_slice_in_dim(total, z * rows, rows, 0)
    own = jnp.where(odd == 1, swapped(own), own)
    states, own = lax.optimization_barrier((states, own))
    limit = clip_rms * math.sqrt(blocks * width)
    weights, factor = pl.pallas_call(
        functools.partial(clip_and_advance, limit),
        out_shape=(
            jax.ShapeDtypeStruct((planes, held, width), jnp.bfloat16),
            jax.ShapeDtypeStruct((8, width), jnp.float32),
        ),
        compiler_params=pltpu.CompilerParams(vmem_limit_bytes=4 << 20),
    )(norms.reshape(planes, cores, width), total, states)

    weights, factor, own, master, first, second, here = lax.optimization_barrier(
        (exchange(weights, ("y", "x")), factor, own, master, first, second, here)
    )
    weights = weights.reshape(planes, line, 1, rows, width)
    mine = jnp.arange(cores) == here
    weights = jnp.where(mine[:, None, None], weights, swapped(weights)).reshape(blocks, width)

    master_new, first_new, second_new = advance(factor[:1] * own, master, first, second)
    first_scale_new = jnp.max(jnp.abs(first_new), axis=1) + 1e-08
    second_scale_new = jnp.max(jnp.abs(second_new), axis=1) + 1e-08
    first_q_new = (first_new / first_scale_new[:, None]).astype(jnp.bfloat16)
    second_q_new = (second_new / second_scale_new[:, None]).astype(jnp.bfloat16)
    return (weights, master_new, first_q_new, first_scale_new, second_q_new, second_scale_new)


def solution(mesh):
    torus = Mesh(mesh.devices.reshape(4, 4, 8, 2), DP)
    in_specs = (P(DP, None, None), P(DP, None), P(DP, None), P(DP), P(DP, None), P(DP))
    out_specs = (P(), P(DP, None), P(DP, None), P(DP), P(DP, None), P(DP))
    return jax.shard_map(
        shards, mesh=torus, in_specs=in_specs, out_specs=out_specs, check_vma=False
    )
```

```python
import functools
import math

import jax
import jax.numpy as jnp
from jax import lax
from jax.experimental import pallas as pl
from jax.experimental.pallas import tpu as pltpu
from jax.sharding import Mesh
from jax.sharding import PartitionSpec as P

DP = ("y", "x", "z", "c")


beta_one = 0.9
beta_two = 0.95
learn_rate = 0.05
decay_rate = 0.1
adam_epsilon = 1e-08
clip_rms = 0.01
first_fix = 1.0 - 0.9**10
second_fix = 1.0 - 0.95**10


def exchange(x, axes):
    return lax.all_to_all(x, axes, split_axis=0, concat_axis=0, tiled=True)


def sent_to_all(x, axes):
    return exchange(jnp.broadcast_to(x, (lax.axis_size(axes), *x.shape)), axes)


def swapped(x):
    return lax.ppermute(x, "c", [(0, 1), (1, 0)])


def from_partner(x, flip):
    line = lax.axis_size("z")
    route = [(2 * z + c, 2 * (z ^ flip) + 1 - c) for z in range(line) for c in range(2)]
    return lax.ppermute(x, ("z", "c"), route)


FLIPS = ((1, 0), (2, 1), (6, 2))


def doubled(x, place, step):
    flip, level = step
    other = from_partner(x, flip)
    mine = jnp.arange(2) == (place[:, None] >> level & 1)
    place = jnp.where(mine, place[:, None], place[:, None] ^ flip).reshape(-1)
    x = jnp.where(mine[:, :, None, None, None], x[:, None], other[:, None])
    return x.reshape(-1, *x.shape[2:]), place


def advance(clipped, master, first, second):
    first_new = beta_one * first + (1.0 - beta_one) * clipped
    second_new = beta_two * second + (1.0 - beta_two) * clipped * clipped
    change = first_new / first_fix / (jnp.sqrt(second_new / second_fix) + adam_epsilon)
    master_new = master * (1.0 - learn_rate * decay_rate) - learn_rate * change
    return master_new, first_new, second_new


def clip_and_advance(limit, norms, total, states, weights, factors):
    pairs = norms[...]
    squares = jnp.sum(pairs[:, 0] + pairs[:, 1], keepdims=True)
    factor = jnp.minimum(1.0, limit / (jnp.sqrt(squares) + 1e-06))
    factors[...] = jnp.broadcast_to(factor, factors.shape)
    line, _, rows, width = states.shape
    for z in range(line):
        place = pl.ds(z * rows, rows)
        new, _, _ = advance(factor * total[place], states[z, 0], states[z, 1], states[z, 2])
        new = new.astype(weights.dtype)
        for plane in range(weights.shape[0]):
            weights[plane, place] = new


def crosswise():
    z = lax.axis_index("z")
    return (z ^ z >> 1) & 1


def lay(other, half, *refs):
    out, sent = refs[-2:]
    side = lax.axis_index("c") ^ crosswise() ^ other
    copy = pltpu.make_async_copy(half, out.at[:, :, side], sent)
    copy.start()
    copy.wait()


def laid(half, other, out):
    planes, line, rows, width = half.shape
    held = () if out is None else (out,)
    return pl.pallas_call(
        functools.partial(lay, other),
        out_shape=jax.ShapeDtypeStruct((planes, line, 2, rows, width), half.dtype),
        in_specs=[pl.BlockSpec(memory_space=pltpu.VMEM)] + [pl.BlockSpec(memory_space=pl.ANY)] * len(held),
        out_specs=pl.BlockSpec(memory_space=pl.ANY),
        scratch_shapes=[pltpu.SemaphoreType.DMA],
        input_output_aliases={1: 0} if held else {},
        compiler_params=pltpu.CompilerParams(vmem_limit_bytes=4 << 20),
    )(half, *held)


def shards(grads, master, first_q, first_scale, second_q, second_scale):
    blocks, width = grads.shape[1:]
    rows = master.shape[0]
    planes, line, cores = lax.axis_size(("y", "x")), lax.axis_size("z"), lax.axis_size("c")
    held = line * rows
    first = first_q.astype(jnp.float32) * first_scale[:, None]
    second = second_q.astype(jnp.float32) * second_scale[:, None]

    z, odd = lax.axis_index("z"), crosswise()
    here = lax.axis_index("c") ^ odd

    arrived = exchange(grads[0].reshape(planes, line * cores * rows, width), ("y", "x"))
    states = jnp.stack([master, first, second])
    states = jnp.where(odd == 1, swapped(states), states)[None]
    place = z[None]
    for step in FLIPS[:0:-1]:
        states, place = doubled(states, place, step)
    arrived, states = lax.optimization_barrier((arrived, states))
    both = arrived.astype(jnp.float32).sum(axis=0).reshape(line, cores, rows, width)
    kept, sent = (lax.dynamic_index_in_dim(both, i, 1, False) for i in (here, 1 - here))
    part = (kept + swapped(sent)).reshape(held, width)

    total, states = lax.optimization_barrier((part, states))
    (last, _), *middle = FLIPS[::-1]
    whole, _ = doubled(states, place, FLIPS[0])
    for flip, _ in middle[::-1]:
        total = total + from_partner(total, flip)
    total, states = lax.optimization_barrier((total, whole))
    total = total + from_partner(total, last)
    norms = sent_to_all(jnp.sum(total * total, axis=0, keepdims=True), ("y", "x", "c"))
    norms, total, states, master, first, second, z, odd = lax.optimization_barrier(
        (norms, total, states, master, first, second, z, odd)
    )
    limit = clip_rms * math.sqrt(blocks * width)
    weights, factor = pl.pallas_call(
        functools.partial(clip_and_advance, limit),
        out_shape=(
            jax.ShapeDtypeStruct((planes, held, width), jnp.bfloat16),
            jax.ShapeDtypeStruct((8, width), jnp.float32),
        ),
        compiler_params=pltpu.CompilerParams(vmem_limit_bytes=4 << 20),
    )(norms.reshape(planes, cores, width), total, states)

    weights, factor, total, master, first, second, z, odd = lax.optimization_barrier(
        (exchange(weights, ("y", "x")), factor, total, master, first, second, z, odd)
    )
    weights = weights.reshape(planes, line, rows, width)
    partner = swapped(weights)
    weights = laid(partner, 1, laid(weights, 0, None)).reshape(blocks, width)

    own = lax.dynamic_slice_in_dim(total, z * rows, rows, 0)
    own = jnp.where(odd == 1, swapped(own), own)
    master_new, first_new, second_new = advance(factor[:1] * own, master, first, second)
    first_scale_new = jnp.max(jnp.abs(first_new), axis=1) + 1e-08
    second_scale_new = jnp.max(jnp.abs(second_new), axis=1) + 1e-08
    first_q_new = (first_new / first_scale_new[:, None]).astype(jnp.bfloat16)
    second_q_new = (second_new / second_scale_new[:, None]).astype(jnp.bfloat16)
    return (weights, master_new, first_q_new, first_scale_new, second_q_new, second_scale_new)


def solution(mesh):
    torus = Mesh(mesh.devices.reshape(4, 4, 8, 2), DP)
    in_specs = (P(DP, None, None), P(DP, None), P(DP, None), P(DP), P(DP, None), P(DP))
    out_specs = (P(), P(DP, None), P(DP, None), P(DP), P(DP, None), P(DP))
    return jax.shard_map(
        shards, mesh=torus, in_specs=in_specs, out_specs=out_specs, check_vma=False
    )
```

```python
import functools
import math

import jax
import jax.numpy as jnp
from jax import lax
from jax.experimental import pallas as pl
from jax.experimental.pallas import tpu as pltpu
from jax.sharding import Mesh
from jax.sharding import PartitionSpec as P

DP = ("y", "x", "z", "c")
PARTS = 4


beta_one = 0.9
beta_two = 0.95
learn_rate = 0.05
decay_rate = 0.1
adam_epsilon = 1e-08
clip_rms = 0.01
first_fix = 1.0 - 0.9**10
second_fix = 1.0 - 0.95**10


def exchange(x, axes):
    return lax.all_to_all(x, axes, split_axis=0, concat_axis=0, tiled=True)


def sent_to_all(x, axes):
    return exchange(jnp.broadcast_to(x, (lax.axis_size(axes), *x.shape)), axes)


def swapped(x):
    return lax.ppermute(x, "c", [(0, 1), (1, 0)])


def from_partner(x, flip):
    return lax.ppermute(x, "z", [(z, z ^ flip) for z in range(lax.axis_size("z"))])


FLIPS = ((1, 0), (2, 1), (6, 2))


def doubled(x, place, step):
    flip, level = step
    other = from_partner(x, flip)
    mine = jnp.arange(2) == (place[:, None] >> level & 1)
    place = jnp.where(mine, place[:, None], place[:, None] ^ flip).reshape(-1)
    x = jnp.where(mine[:, :, None, None, None], x[:, None], other[:, None])
    return x.reshape(-1, *x.shape[2:]), place


def advance(clipped, master, first, second):
    first_new = beta_one * first + (1.0 - beta_one) * clipped
    second_new = beta_two * second + (1.0 - beta_two) * clipped * clipped
    change = first_new / first_fix / (jnp.sqrt(second_new / second_fix) + adam_epsilon)
    master_new = master * (1.0 - learn_rate * decay_rate) - learn_rate * change
    return master_new, first_new, second_new


def clip_and_advance(limit, norms, total, states, weights, factors):
    squares = jnp.sum(norms[...], axis=0)
    factor = jnp.minimum(1.0, limit / (jnp.sqrt(jnp.sum(squares, axis=1, keepdims=True)) + 1e-06))
    factors[...] = jnp.broadcast_to(factor, factors.shape)
    line, _, rows, width = states.shape
    for z in range(line):
        place = pl.ds(z * rows, rows)
        new, _, _ = advance(factor * total[place], states[z, 0], states[z, 1], states[z, 2])
        new = new.astype(weights.dtype)
        for plane in range(weights.shape[0]):
            weights[plane, place] = new


def copies_of_half(half, out, other, sent):
    side = lax.axis_index("c") ^ other
    planes = half.shape[0] // PARTS
    spans = [pl.ds(part * planes, planes) for part in range(PARTS)]
    return [
        pltpu.make_async_copy(half.at[span], out.at[span, :, side], sent.at[part])
        for part, span in enumerate(spans)
    ]


def lay_and_advance(half, factor, total, states, out, *refs):
    results, held, sent = refs[:5], refs[5:10], refs[10]
    copies = copies_of_half(half, out, 0, sent)
    for copy in copies:
        copy.start()

    rows = states.shape[2]
    z = lax.axis_index("z")
    own = total[pl.ds(pl.multiple_of(z * rows, rows), rows)]
    held[0][...], *new = advance(factor[:1] * own, states[z, 0], states[z, 1], states[z, 2])
    square = (rows, rows)
    diagonal = lax.broadcasted_iota(jnp.int32, square, 0) == lax.broadcasted_iota(jnp.int32, square, 1)
    for moment, quotient, scale in zip(new, held[1::2], held[2::2]):
        largest = jnp.max(jnp.abs(moment), axis=1, keepdims=True) + 1e-08
        quotient[...] = (moment / largest).astype(quotient.dtype)
        scale[...] = jnp.sum(jnp.where(diagonal, largest, 0.0), axis=0, keepdims=True)
    for i, (result, kept) in enumerate(zip(results, held)):
        copies.append(pltpu.make_async_copy(kept, result, sent.at[PARTS + i]))
        copies[-1].start()
    for copy in copies:
        copy.wait()


def lay_other(half, _, out, sent):
    copies = copies_of_half(half, out, 1, sent)
    for copy in copies:
        copy.start()
    for copy in copies:
        copy.wait()


def shards(grads, master, first_q, first_scale, second_q, second_scale):
    blocks, width = grads.shape[1:]
    rows = master.shape[0]
    planes, line, cores = lax.axis_size(("y", "x")), lax.axis_size("z"), lax.axis_size("c")
    held = line * rows
    first = first_q.astype(jnp.float32) * first_scale[:, None]
    second = second_q.astype(jnp.float32) * second_scale[:, None]

    here = lax.axis_index("c")

    arrived = exchange(grads[0].reshape(planes, line * cores * rows, width), ("y", "x"))
    states = jnp.stack([master, first, second])[None]
    place = lax.axis_index("z")[None]
    for step in FLIPS[:0:-1]:
        states, place = doubled(states, place, step)
    arrived, states = lax.optimization_barrier((arrived, states))
    both = arrived.astype(jnp.float32).sum(axis=0).reshape(line, cores, rows, width)
    kept, sent = (lax.dynamic_index_in_dim(both, i, 1, False) for i in (here, 1 - here))
    part = (kept + swapped(sent)).reshape(held, width)

    total, states = lax.optimization_barrier((part, states))
    (last, _), *middle = FLIPS[::-1]
    whole, _ = doubled(states, place, FLIPS[0])
    for flip, _ in middle[::-1]:
        total = total + from_partner(total, flip)
    total, states = lax.optimization_barrier((total, whole))
    total = total + from_partner(total, last)
    norms = sent_to_all(jnp.sum(total * total, axis=0, keepdims=True), ("y", "x", "c"))
    norms, total, states = lax.optimization_barrier((norms, total, states))
    small = pltpu.CompilerParams(vmem_limit_bytes=4 << 20)
    weights, factor = pl.pallas_call(
        functools.partial(clip_and_advance, clip_rms * math.sqrt(blocks * width)),
        out_shape=(
            jax.ShapeDtypeStruct((planes, held, width), jnp.bfloat16),
            jax.ShapeDtypeStruct((8, width), jnp.float32),
        ),
        compiler_params=small,
    )(norms, total, states)

    weights, factor, total, states = lax.optimization_barrier(
        (exchange(weights, ("y", "x")), factor, total, states)
    )
    weights = weights.reshape(planes, line, rows, width)
    partner = swapped(weights)
    whole = jax.ShapeDtypeStruct((planes, line, cores, rows, width), jnp.bfloat16)
    own, scale = (rows, width), (1, rows)
    results = [(own, jnp.float32)] + [(own, jnp.bfloat16), (scale, jnp.float32)] * 2
    vmem, anywhere = (pl.BlockSpec(memory_space=space) for space in (pltpu.VMEM, pl.ANY))
    weights, *results = pl.pallas_call(
        lay_and_advance,
        out_shape=[whole] + [jax.ShapeDtypeStruct(*result) for result in results],
        in_specs=[vmem] * 4,
        out_specs=[anywhere] * 6,
        scratch_shapes=[pltpu.VMEM(*result) for result in results] + [pltpu.SemaphoreType.DMA((PARTS + 5,))],
        compiler_params=small,
    )(weights, factor, total, states)
    weights = pl.pallas_call(
        lay_other,
        out_shape=whole,
        in_specs=[vmem, anywhere],
        out_specs=anywhere,
        scratch_shapes=[pltpu.SemaphoreType.DMA((PARTS,))],
        input_output_aliases={1: 0},
        compiler_params=small,
    )(partner, weights)
    master_new, first_q_new, first_scale_new, second_q_new, second_scale_new = results
    weights = weights.reshape(blocks, width)
    return (weights, master_new, first_q_new, first_scale_new[0], second_q_new, second_scale_new[0])


def solution(mesh):
    torus = Mesh(mesh.devices.reshape(4, 4, 8, 2), DP)
    in_specs = (P(DP, None, None), P(DP, None), P(DP, None), P(DP), P(DP, None), P(DP))
    out_specs = (P(), P(DP, None), P(DP, None), P(DP), P(DP, None), P(DP))
    return jax.shard_map(
        shards, mesh=torus, in_specs=in_specs, out_specs=out_specs, check_vma=False
    )
```

```python
import functools
import math

import jax
import jax.numpy as jnp
from jax import lax
from jax.experimental import pallas as pl
from jax.experimental.pallas import tpu as pltpu
from jax.sharding import Mesh
from jax.sharding import PartitionSpec as P

DP = ("y", "x", "z", "c")
PARTS = 4


beta_one = 0.9
beta_two = 0.95
learn_rate = 0.05
decay_rate = 0.1
adam_epsilon = 1e-08
clip_rms = 0.01
first_fix = 1.0 - 0.9**10
second_fix = 1.0 - 0.95**10


def exchange(x, axes):
    return lax.all_to_all(x, axes, split_axis=0, concat_axis=0, tiled=True)


def sent_to_all(x, axes):
    return exchange(jnp.broadcast_to(x, (lax.axis_size(axes), *x.shape)), axes)


def swapped(x):
    return lax.ppermute(x, "c", [(0, 1), (1, 0)])


def from_partner(x, flip):
    return lax.ppermute(x, "z", [(z, z ^ flip) for z in range(lax.axis_size("z"))])


FLIPS = ((1, 0), (2, 1), (6, 2))


def doubled(x, place, step):
    flip, level = step
    other = from_partner(x, flip)
    mine = jnp.arange(2) == (place[:, None] >> level & 1)
    place = jnp.where(mine, place[:, None], place[:, None] ^ flip).reshape(-1)
    x = jnp.where(mine[:, :, None, None, None], x[:, None], other[:, None])
    return x.reshape(-1, *x.shape[2:]), place


def advance(clipped, master, first, second):
    first_new = beta_one * first + (1.0 - beta_one) * clipped
    second_new = beta_two * second + (1.0 - beta_two) * clipped * clipped
    change = first_new / first_fix / (jnp.sqrt(second_new / second_fix) + adam_epsilon)
    master_new = master * (1.0 - learn_rate * decay_rate) - learn_rate * change
    return master_new, first_new, second_new


def clip_and_advance(limit, norms, total, states, weights, factors):
    squares = jnp.sum(norms[...], axis=0)
    factor = jnp.minimum(1.0, limit / (jnp.sqrt(jnp.sum(squares, axis=1, keepdims=True)) + 1e-06))
    factors[...] = jnp.broadcast_to(factor, factors.shape)
    line, _, rows, width = states.shape
    for z in range(line):
        place = pl.ds(z * rows, rows)
        new, _, _ = advance(factor * total[place], states[z, 0], states[z, 1], states[z, 2])
        new = new.astype(weights.dtype)
        for plane in range(weights.shape[0]):
            weights[plane, place] = new


def copies_of_half(half, out, other, sent):
    side = lax.axis_index("c") ^ other
    planes = half.shape[0] // PARTS
    spans = [pl.ds(part * planes, planes) for part in range(PARTS)]
    return [
        pltpu.make_async_copy(half.at[span], out.at[span, :, side], sent.at[part])
        for part, span in enumerate(spans)
    ]


def lay_and_advance(half, factor, total, states, out, *refs):
    results, held, sent = refs[:5], refs[5:10], refs[10]
    copies = copies_of_half(half, out, 0, sent)
    for copy in copies:
        copy.start()

    rows = states.shape[2]
    z = lax.axis_index("z")
    own = total[pl.ds(pl.multiple_of(z * rows, rows), rows)]
    held[0][...], *new = advance(factor[:1] * own, states[z, 0], states[z, 1], states[z, 2])
    square = (rows, rows)
    diagonal = lax.broadcasted_iota(jnp.int32, square, 0) == lax.broadcasted_iota(jnp.int32, square, 1)
    for moment, quotient, scale in zip(new, held[1::2], held[2::2]):
        largest = jnp.max(jnp.abs(moment), axis=1, keepdims=True) + 1e-08
        quotient[...] = (moment / largest).astype(quotient.dtype)
        scale[...] = jnp.sum(jnp.where(diagonal, largest, 0.0), axis=0, keepdims=True)
    for i, (result, kept) in enumerate(zip(results, held)):
        copies.append(pltpu.make_async_copy(kept, result, sent.at[PARTS + i]))
        copies[-1].start()
    for copy in copies:
        copy.wait()


def lay_other(half, _, out, sent):
    copies = copies_of_half(half, out, 1, sent)
    for copy in copies:
        copy.start()
    for copy in copies:
        copy.wait()


def shards(grads, master, first_q, first_scale, second_q, second_scale):
    blocks, width = grads.shape[1:]
    rows = master.shape[0]
    planes, line, cores = lax.axis_size(("y", "x")), lax.axis_size("z"), lax.axis_size("c")
    held = line * rows
    first = first_q.astype(jnp.float32) * first_scale[:, None]
    second = second_q.astype(jnp.float32) * second_scale[:, None]

    here = lax.axis_index("c")

    arrived = exchange(grads[0].reshape(planes, line * cores * rows, width), ("y", "x"))
    states = jnp.stack([master, first, second])[None]
    place = lax.axis_index("z")[None]
    for step in FLIPS[:0:-1]:
        states, place = doubled(states, place, step)
    arrived, states = lax.optimization_barrier((arrived, states))
    both = arrived.astype(jnp.float32).sum(axis=0).reshape(line, cores, rows, width)
    kept, sent = (lax.dynamic_index_in_dim(both, i, 1, False) for i in (here, 1 - here))
    part = (kept + swapped(sent)).reshape(held, width)

    total, states = lax.optimization_barrier((part, states))
    whole, _ = doubled(states, place, FLIPS[0])
    total = total + from_partner(total, 1)
    others = [from_partner(total, flip) for flip in (2, 6, 4)]
    others, states = lax.optimization_barrier((others, whole))
    total = (total + others[0]) + (others[1] + others[2])
    norms = sent_to_all(jnp.sum(total * total, axis=0, keepdims=True), ("y", "x", "c"))
    norms, total, states = lax.optimization_barrier((norms, total, states))
    small = pltpu.CompilerParams(vmem_limit_bytes=4 << 20)
    weights, factor = pl.pallas_call(
        functools.partial(clip_and_advance, clip_rms * math.sqrt(blocks * width)),
        out_shape=(
            jax.ShapeDtypeStruct((planes, held, width), jnp.bfloat16),
            jax.ShapeDtypeStruct((8, width), jnp.float32),
        ),
        compiler_params=small,
    )(norms, total, states)

    weights, factor, total, states = lax.optimization_barrier(
        (exchange(weights, ("y", "x")), factor, total, states)
    )
    weights = weights.reshape(planes, line, rows, width)
    partner = swapped(weights)
    whole = jax.ShapeDtypeStruct((planes, line, cores, rows, width), jnp.bfloat16)
    own, scale = (rows, width), (1, rows)
    results = [(own, jnp.float32)] + [(own, jnp.bfloat16), (scale, jnp.float32)] * 2
    vmem, anywhere = (pl.BlockSpec(memory_space=space) for space in (pltpu.VMEM, pl.ANY))
    weights, *results = pl.pallas_call(
        lay_and_advance,
        out_shape=[whole] + [jax.ShapeDtypeStruct(*result) for result in results],
        in_specs=[vmem] * 4,
        out_specs=[anywhere] * 6,
        scratch_shapes=[pltpu.VMEM(*result) for result in results] + [pltpu.SemaphoreType.DMA((PARTS + 5,))],
        compiler_params=small,
    )(weights, factor, total, states)
    weights = pl.pallas_call(
        lay_other,
        out_shape=whole,
        in_specs=[vmem, anywhere],
        out_specs=anywhere,
        scratch_shapes=[pltpu.SemaphoreType.DMA((PARTS,))],
        input_output_aliases={1: 0},
        compiler_params=small,
    )(partner, weights)
    master_new, first_q_new, first_scale_new, second_q_new, second_scale_new = results
    weights = weights.reshape(blocks, width)
    return (weights, master_new, first_q_new, first_scale_new[0], second_q_new, second_scale_new[0])


def solution(mesh):
    torus = Mesh(mesh.devices.reshape(4, 4, 8, 2), DP)
    in_specs = (P(DP, None, None), P(DP, None), P(DP, None), P(DP), P(DP, None), P(DP))
    out_specs = (P(), P(DP, None), P(DP, None), P(DP), P(DP, None), P(DP))
    return jax.shard_map(
        shards, mesh=torus, in_specs=in_specs, out_specs=out_specs, check_vma=False
    )
```

```python
import functools
import math

import jax
import jax.numpy as jnp
from jax import lax
from jax.experimental import pallas as pl
from jax.experimental.pallas import tpu as pltpu
from jax.sharding import Mesh
from jax.sharding import PartitionSpec as P

DP = ("y", "x", "z", "c")
PARTS = 4


beta_one = 0.9
beta_two = 0.95
learn_rate = 0.05
decay_rate = 0.1
adam_epsilon = 1e-08
clip_rms = 0.01
first_fix = 1.0 - 0.9**10
second_fix = 1.0 - 0.95**10


def exchange(x, axes):
    return lax.all_to_all(x, axes, split_axis=0, concat_axis=0, tiled=True)


def sent_to_all(x, axes):
    return exchange(jnp.broadcast_to(x, (lax.axis_size(axes), *x.shape)), axes)


def swapped(x):
    return lax.ppermute(x, "c", [(0, 1), (1, 0)])


def from_partner(x, flip):
    return lax.ppermute(x, "z", [(z, z ^ flip) for z in range(lax.axis_size("z"))])


def placed(pieces, bits):
    if len(pieces) == 1:
        return pieces
    half = len(pieces) // 2
    low, high = placed(pieces[:half], bits[1:]), placed(pieces[half:], bits[1:])
    lower = [jnp.where(bits[0] == 1, b, a) for a, b in zip(low, high)]
    upper = [jnp.where(bits[0] == 1, a, b) for a, b in zip(low, high)]
    return lower + upper


def gathered(x):
    z = lax.axis_index("z")
    bits = [z >> level & 1 for level in (2, 1, 0)]
    pieces = [x] + [from_partner(x, flip) for flip in (2, 4, 6)]
    apart = jnp.stack(placed(pieces, bits[:2]))
    pair = placed([apart, from_partner(apart, 1)], bits[2:])
    return jnp.stack(pair, axis=1).reshape(-1, *x.shape)


def advance(clipped, master, first, second):
    first_new = beta_one * first + (1.0 - beta_one) * clipped
    second_new = beta_two * second + (1.0 - beta_two) * clipped * clipped
    change = first_new / first_fix / (jnp.sqrt(second_new / second_fix) + adam_epsilon)
    master_new = master * (1.0 - learn_rate * decay_rate) - learn_rate * change
    return master_new, first_new, second_new


def clip_and_advance(limit, norms, total, states, weights, factors):
    squares = jnp.sum(norms[...], axis=0)
    factor = jnp.minimum(1.0, limit / (jnp.sqrt(jnp.sum(squares, axis=1, keepdims=True)) + 1e-06))
    factors[...] = jnp.broadcast_to(factor, factors.shape)
    line, _, rows, width = states.shape
    for z in range(line):
        place = pl.ds(z * rows, rows)
        new, _, _ = advance(factor * total[place], states[z, 0], states[z, 1], states[z, 2])
        new = new.astype(weights.dtype)
        for plane in range(weights.shape[0]):
            weights[plane, place] = new


def copies_of_half(half, out, other, sent):
    side = lax.axis_index("c") ^ other
    planes = half.shape[0] // PARTS
    spans = [pl.ds(part * planes, planes) for part in range(PARTS)]
    return [
        pltpu.make_async_copy(half.at[span], out.at[span, :, side], sent.at[part])
        for part, span in enumerate(spans)
    ]


def lay_and_advance(half, factor, total, states, out, *refs):
    results, held, sent = refs[:5], refs[5:10], refs[10]
    copies = copies_of_half(half, out, 0, sent)
    for copy in copies:
        copy.start()

    rows = states.shape[2]
    z = lax.axis_index("z")
    own = total[pl.ds(pl.multiple_of(z * rows, rows), rows)]
    held[0][...], *new = advance(factor[:1] * own, states[z, 0], states[z, 1], states[z, 2])
    square = (rows, rows)
    diagonal = lax.broadcasted_iota(jnp.int32, square, 0) == lax.broadcasted_iota(jnp.int32, square, 1)
    for moment, quotient, scale in zip(new, held[1::2], held[2::2]):
        largest = jnp.max(jnp.abs(moment), axis=1, keepdims=True) + 1e-08
        quotient[...] = (moment / largest).astype(quotient.dtype)
        scale[...] = jnp.sum(jnp.where(diagonal, largest, 0.0), axis=0, keepdims=True)
    for i, (result, kept) in enumerate(zip(results, held)):
        copies.append(pltpu.make_async_copy(kept, result, sent.at[PARTS + i]))
        copies[-1].start()
    for copy in copies:
        copy.wait()


def lay_other(half, _, out, sent):
    copies = copies_of_half(half, out, 1, sent)
    for copy in copies:
        copy.start()
    for copy in copies:
        copy.wait()


def shards(grads, master, first_q, first_scale, second_q, second_scale):
    blocks, width = grads.shape[1:]
    rows = master.shape[0]
    planes, line, cores = lax.axis_size(("y", "x")), lax.axis_size("z"), lax.axis_size("c")
    held = line * rows
    first = first_q.astype(jnp.float32) * first_scale[:, None]
    second = second_q.astype(jnp.float32) * second_scale[:, None]

    here = lax.axis_index("c")

    arrived = exchange(grads[0].reshape(planes, line * cores * rows, width), ("y", "x"))
    states = gathered(jnp.stack([master, first, second]))
    arrived, states = lax.optimization_barrier((arrived, states))
    both = arrived.astype(jnp.float32).sum(axis=0).reshape(line, cores, rows, width)
    kept, sent = (lax.dynamic_index_in_dim(both, i, 1, False) for i in (here, 1 - here))
    part = (kept + swapped(sent)).reshape(held, width)

    total = part + from_partner(part, 1)
    others = [from_partner(total, flip) for flip in (2, 6, 4)]
    total = (total + others[0]) + (others[1] + others[2])
    norms = sent_to_all(jnp.sum(total * total, axis=0, keepdims=True), ("y", "x", "c"))
    norms, total, states = lax.optimization_barrier((norms, total, states))
    small = pltpu.CompilerParams(vmem_limit_bytes=4 << 20)
    weights, factor = pl.pallas_call(
        functools.partial(clip_and_advance, clip_rms * math.sqrt(blocks * width)),
        out_shape=(
            jax.ShapeDtypeStruct((planes, held, width), jnp.bfloat16),
            jax.ShapeDtypeStruct((8, width), jnp.float32),
        ),
        compiler_params=small,
    )(norms, total, states)

    weights, factor, total, states = lax.optimization_barrier(
        (exchange(weights, ("y", "x")), factor, total, states)
    )
    weights = weights.reshape(planes, line, rows, width)
    partner = swapped(weights)
    whole = jax.ShapeDtypeStruct((planes, line, cores, rows, width), jnp.bfloat16)
    own, scale = (rows, width), (1, rows)
    results = [(own, jnp.float32)] + [(own, jnp.bfloat16), (scale, jnp.float32)] * 2
    vmem, anywhere = (pl.BlockSpec(memory_space=space) for space in (pltpu.VMEM, pl.ANY))
    weights, *results = pl.pallas_call(
        lay_and_advance,
        out_shape=[whole] + [jax.ShapeDtypeStruct(*result) for result in results],
        in_specs=[vmem] * 4,
        out_specs=[anywhere] * 6,
        scratch_shapes=[pltpu.VMEM(*result) for result in results] + [pltpu.SemaphoreType.DMA((PARTS + 5,))],
        compiler_params=small,
    )(weights, factor, total, states)
    weights = pl.pallas_call(
        lay_other,
        out_shape=whole,
        in_specs=[vmem, anywhere],
        out_specs=anywhere,
        scratch_shapes=[pltpu.SemaphoreType.DMA((PARTS,))],
        input_output_aliases={1: 0},
        compiler_params=small,
    )(partner, weights)
    master_new, first_q_new, first_scale_new, second_q_new, second_scale_new = results
    weights = weights.reshape(blocks, width)
    return (weights, master_new, first_q_new, first_scale_new[0], second_q_new, second_scale_new[0])


def solution(mesh):
    torus = Mesh(mesh.devices.reshape(4, 4, 8, 2), DP)
    in_specs = (P(DP, None, None), P(DP, None), P(DP, None), P(DP), P(DP, None), P(DP))
    out_specs = (P(), P(DP, None), P(DP, None), P(DP), P(DP, None), P(DP))
    return jax.shard_map(
        shards, mesh=torus, in_specs=in_specs, out_specs=out_specs, check_vma=False
    )
```

```python
import functools
import math

import jax
import jax.numpy as jnp
from jax import lax
from jax.experimental import pallas as pl
from jax.experimental.pallas import tpu as pltpu
from jax.sharding import Mesh
from jax.sharding import PartitionSpec as P

DP = ("y", "x", "z", "c")
PARTS = 4


beta_one = 0.9
beta_two = 0.95
learn_rate = 0.05
decay_rate = 0.1
adam_epsilon = 1e-08
clip_rms = 0.01
first_fix = 1.0 - 0.9**10
second_fix = 1.0 - 0.95**10


def exchange(x, axes):
    return lax.all_to_all(x, axes, split_axis=0, concat_axis=0, tiled=True)


def sent_to_all(x, axes):
    return exchange(jnp.broadcast_to(x, (lax.axis_size(axes), *x.shape)), axes)


def swapped(x):
    return lax.ppermute(x, "c", [(0, 1), (1, 0)])


def from_partner(x, flip):
    return lax.ppermute(x, "z", [(z, z ^ flip) for z in range(lax.axis_size("z"))])


def doubled(x, place, step):
    flip, level = step
    other = from_partner(x, flip)
    mine = jnp.arange(2) == (place[:, None] >> level & 1)
    place = jnp.where(mine, place[:, None], place[:, None] ^ flip).reshape(-1)
    x = jnp.where(mine.reshape(mine.shape + (1,) * (x.ndim - 1)), x[:, None], other[:, None])
    return x.reshape(-1, *x.shape[2:]), place


def advance(clipped, master, first, second):
    first_new = beta_one * first + (1.0 - beta_one) * clipped
    second_new = beta_two * second + (1.0 - beta_two) * clipped * clipped
    change = first_new / first_fix / (jnp.sqrt(second_new / second_fix) + adam_epsilon)
    master_new = master * (1.0 - learn_rate * decay_rate) - learn_rate * change
    return master_new, first_new, second_new


def clip_and_advance(limit, norms, total, states, weights, factors):
    squares = jnp.sum(norms[...], axis=0)
    factor = jnp.minimum(1.0, limit / (jnp.sqrt(jnp.sum(squares, axis=1, keepdims=True)) + 1e-06))
    factors[...] = jnp.broadcast_to(factor, factors.shape)
    line, _, rows, width = states.shape
    for z in range(line):
        place = pl.ds(z * rows, rows)
        new, _, _ = advance(factor * total[place], states[z, 0], states[z, 1], states[z, 2])
        new = new.astype(weights.dtype)
        for plane in range(weights.shape[0]):
            weights[plane, place] = new


def copies_of_half(half, out, other, sent):
    side = lax.axis_index("c") ^ other
    planes = half.shape[0] // PARTS
    spans = [pl.ds(part * planes, planes) for part in range(PARTS)]
    return [
        pltpu.make_async_copy(half.at[span], out.at[span, side], sent.at[part])
        for part, span in enumerate(spans)
    ]


def lay_and_advance(half, factor, own, states, out, *refs):
    results, held, sent = refs[:5], refs[5:10], refs[10]
    copies = copies_of_half(half, out, 0, sent)
    for copy in copies:
        copy.start()

    rows = own.shape[0]
    held[0][...], *new = advance(factor[:1] * own[...], states[0], states[1], states[2])
    square = (rows, rows)
    diagonal = lax.broadcasted_iota(jnp.int32, square, 0) == lax.broadcasted_iota(jnp.int32, square, 1)
    for moment, quotient, scale in zip(new, held[1::2], held[2::2]):
        largest = jnp.max(jnp.abs(moment), axis=1, keepdims=True) + 1e-08
        quotient[...] = (moment / largest).astype(quotient.dtype)
        scale[...] = jnp.sum(jnp.where(diagonal, largest, 0.0), axis=0, keepdims=True)
    for i, (result, kept) in enumerate(zip(results, held)):
        copies.append(pltpu.make_async_copy(kept, result, sent.at[PARTS + i]))
        copies[-1].start()
    for copy in copies:
        copy.wait()


def lay_other(half, _, out, sent):
    copies = copies_of_half(half, out, 1, sent)
    for copy in copies:
        copy.start()
    for copy in copies:
        copy.wait()


def shards(grads, master, first_q, first_scale, second_q, second_scale):
    blocks, width = grads.shape[1:]
    rows = master.shape[0]
    planes, line, cores = lax.axis_size(("y", "x")), lax.axis_size("z"), lax.axis_size("c")
    held = line * rows
    first = first_q.astype(jnp.float32) * first_scale[:, None]
    second = second_q.astype(jnp.float32) * second_scale[:, None]

    z, core = lax.axis_index("z"), lax.axis_index("c")
    near = z // (line // cores) == core
    chunks = line // cores * cores

    arrived = exchange(grads[0].reshape(planes * cores, held, width), ("y", "x", "c"))
    kept = jnp.stack([master, first, second])
    chip = jnp.where((jnp.arange(cores) == core)[:, None, None, None], kept, swapped(kept))
    states = jnp.where(near, chip, from_partner(chip, 6))[None]
    place = jnp.where(near, z, z ^ 6)[None]
    states, place = doubled(states, place, (2, 1))
    arrived, states = lax.optimization_barrier((arrived, states))
    part = arrived.astype(jnp.float32).sum(axis=0)

    total, states = lax.optimization_barrier((part, states))
    whole, _ = doubled(states, place, (1, 0))
    total = total + from_partner(total, 1)
    others = [from_partner(total, flip) for flip in (2, 6, 4)]
    others, states = lax.optimization_barrier((others, whole))
    total = (total + others[0]) + (others[1] + others[2])
    states = states.reshape(chunks, 3, rows, width)
    norms = sent_to_all(jnp.sum(total * total, axis=0, keepdims=True), ("y", "x", "c"))
    norms, total, states = lax.optimization_barrier((norms, total, states))
    small = pltpu.CompilerParams(vmem_limit_bytes=4 << 20)
    weights, factor = pl.pallas_call(
        functools.partial(clip_and_advance, clip_rms * math.sqrt(blocks * width)),
        out_shape=(
            jax.ShapeDtypeStruct((planes, held, width), jnp.bfloat16),
            jax.ShapeDtypeStruct((8, width), jnp.float32),
        ),
        compiler_params=small,
    )(norms, total, states)

    weights, factor, total, kept, z = lax.optimization_barrier(
        (exchange(weights, ("y", "x")), factor, total, kept, z)
    )
    partner = swapped(weights)
    pieces = total.reshape(line // cores, cores, rows, width)[z % (line // cores)]
    mine, other = (lax.dynamic_index_in_dim(pieces, i, 0, False) for i in (core, 1 - core))
    own_total = jnp.where(near, mine, swapped(other))
    whole = jax.ShapeDtypeStruct((planes, cores, held, width), jnp.bfloat16)
    own, scale = (rows, width), (1, rows)
    results = [(own, jnp.float32)] + [(own, jnp.bfloat16), (scale, jnp.float32)] * 2
    vmem, anywhere = (pl.BlockSpec(memory_space=space) for space in (pltpu.VMEM, pl.ANY))
    weights, *results = pl.pallas_call(
        lay_and_advance,
        out_shape=[whole] + [jax.ShapeDtypeStruct(*result) for result in results],
        in_specs=[vmem] * 4,
        out_specs=[anywhere] * 6,
        scratch_shapes=[pltpu.VMEM(*result) for result in results] + [pltpu.SemaphoreType.DMA((PARTS + 5,))],
        compiler_params=small,
    )(weights, factor, own_total, kept)
    weights = pl.pallas_call(
        lay_other,
        out_shape=whole,
        in_specs=[vmem, anywhere],
        out_specs=anywhere,
        scratch_shapes=[pltpu.SemaphoreType.DMA((PARTS,))],
        input_output_aliases={1: 0},
        compiler_params=small,
    )(partner, weights)
    master_new, first_q_new, first_scale_new, second_q_new, second_scale_new = results
    weights = weights.reshape(blocks, width)
    return (weights, master_new, first_q_new, first_scale_new[0], second_q_new, second_scale_new[0])


def solution(mesh):
    torus = Mesh(mesh.devices.reshape(4, 4, 8, 2), DP)
    in_specs = (P(DP, None, None), P(DP, None), P(DP, None), P(DP), P(DP, None), P(DP))
    out_specs = (P(), P(DP, None), P(DP, None), P(DP), P(DP, None), P(DP))
    return jax.shard_map(
        shards, mesh=torus, in_specs=in_specs, out_specs=out_specs, check_vma=False
    )
```

```python
import functools
import math

import jax
import jax.numpy as jnp
from jax import lax
from jax.experimental import pallas as pl
from jax.experimental.pallas import tpu as pltpu
from jax.sharding import Mesh
from jax.sharding import PartitionSpec as P

DP = ("y", "x", "z", "c")
PARTS = 4


beta_one = 0.9
beta_two = 0.95
learn_rate = 0.05
decay_rate = 0.1
adam_epsilon = 1e-08
clip_rms = 0.01
first_fix = 1.0 - 0.9**10
second_fix = 1.0 - 0.95**10


def exchange(x, axes):
    return lax.all_to_all(x, axes, split_axis=0, concat_axis=0, tiled=True)


def sent_to_all(x, axes):
    return exchange(jnp.broadcast_to(x, (lax.axis_size(axes), *x.shape)), axes)


def swapped(x):
    return lax.ppermute(x, "c", [(0, 1), (1, 0)])


def from_partner(x, flip):
    return lax.ppermute(x, "z", [(z, z ^ flip) for z in range(lax.axis_size("z"))])


def doubled(x, place, step):
    flip, level = step
    other = from_partner(x, flip)
    mine = jnp.arange(2) == (place[:, None] >> level & 1)
    place = jnp.where(mine, place[:, None], place[:, None] ^ flip).reshape(-1)
    x = jnp.where(mine.reshape(mine.shape + (1,) * (x.ndim - 1)), x[:, None], other[:, None])
    return x.reshape(-1, *x.shape[2:]), place


def advance(clipped, master, first, second):
    first_new = beta_one * first + (1.0 - beta_one) * clipped
    second_new = beta_two * second + (1.0 - beta_two) * clipped * clipped
    change = first_new / first_fix / (jnp.sqrt(second_new / second_fix) + adam_epsilon)
    master_new = master * (1.0 - learn_rate * decay_rate) - learn_rate * change
    return master_new, first_new, second_new


def clip_and_advance(limit, norms, total, states, weights, factors):
    squares = jnp.sum(norms[...], axis=0)
    factor = jnp.minimum(1.0, limit / (jnp.sqrt(jnp.sum(squares, axis=1, keepdims=True)) + 1e-06))
    factors[...] = jnp.broadcast_to(factor, factors.shape)
    line, _, rows, width = states.shape
    for z in range(line):
        place = pl.ds(z * rows, rows)
        new, _, _ = advance(factor * total[place], states[z, 0], states[z, 1], states[z, 2])
        new = new.astype(weights.dtype)
        for plane in range(weights.shape[0]):
            weights[plane, place] = new


def copies_of_half(half, out, other, sent):
    side = lax.axis_index("c") ^ other
    planes = half.shape[0] // PARTS
    spans = [pl.ds(part * planes, planes) for part in range(PARTS)]
    return [
        pltpu.make_async_copy(half.at[span], out.at[span, side], sent.at[part])
        for part, span in enumerate(spans)
    ]


def lay(half, out, sent):
    copies = copies_of_half(half, out, 0, sent)
    for copy in copies:
        copy.start()
    for copy in copies:
        copy.wait()


def lay_and_advance(half, factor, own, states, _, out, *refs):
    results, held, sent = refs[:5], refs[5:10], refs[10]
    copies = copies_of_half(half, out, 1, sent)
    for copy in copies:
        copy.start()

    rows = own.shape[0]
    held[0][...], *new = advance(factor[:1] * own[...], states[0], states[1], states[2])
    square = (rows, rows)
    diagonal = lax.broadcasted_iota(jnp.int32, square, 0) == lax.broadcasted_iota(jnp.int32, square, 1)
    for moment, quotient, scale in zip(new, held[1::2], held[2::2]):
        largest = jnp.max(jnp.abs(moment), axis=1, keepdims=True) + 1e-08
        quotient[...] = (moment / largest).astype(quotient.dtype)
        scale[...] = jnp.sum(jnp.where(diagonal, largest, 0.0), axis=0, keepdims=True)
    for i, (result, kept) in enumerate(zip(results, held)):
        copies.append(pltpu.make_async_copy(kept, result, sent.at[PARTS + i]))
        copies[-1].start()
    for copy in copies:
        copy.wait()


def shards(grads, master, first_q, first_scale, second_q, second_scale):
    blocks, width = grads.shape[1:]
    rows = master.shape[0]
    planes, line, cores = lax.axis_size(("y", "x")), lax.axis_size("z"), lax.axis_size("c")
    held = line * rows
    first = first_q.astype(jnp.float32) * first_scale[:, None]
    second = second_q.astype(jnp.float32) * second_scale[:, None]

    z, core = lax.axis_index("z"), lax.axis_index("c")
    near = z // (line // cores) == core
    chunks = line // cores * cores

    arrived = exchange(grads[0].reshape(planes * cores, held, width), ("y", "x", "c"))
    kept = jnp.stack([master, first, second])
    chip = jnp.where((jnp.arange(cores) == core)[:, None, None, None], kept, swapped(kept))
    states = jnp.where(near, chip, from_partner(chip, 6))[None]
    place = jnp.where(near, z, z ^ 6)[None]
    states, place = doubled(states, place, (2, 1))
    arrived, states = lax.optimization_barrier((arrived, states))
    part = arrived.astype(jnp.float32).sum(axis=0)

    total, states = lax.optimization_barrier((part, states))
    whole, _ = doubled(states, place, (1, 0))
    total = total + from_partner(total, 1)
    others = [from_partner(total, flip) for flip in (2, 6, 4)]
    others, states = lax.optimization_barrier((others, whole))
    total = (total + others[0]) + (others[1] + others[2])
    states = states.reshape(chunks, 3, rows, width)
    norms = sent_to_all(jnp.sum(total * total, axis=0, keepdims=True), ("y", "x", "c"))
    norms, total, states = lax.optimization_barrier((norms, total, states))
    small = pltpu.CompilerParams(vmem_limit_bytes=4 << 20)
    weights, factor = pl.pallas_call(
        functools.partial(clip_and_advance, clip_rms * math.sqrt(blocks * width)),
        out_shape=(
            jax.ShapeDtypeStruct((planes, held, width), jnp.bfloat16),
            jax.ShapeDtypeStruct((8, width), jnp.float32),
        ),
        compiler_params=small,
    )(norms, total, states)

    weights, factor, total, kept, z = lax.optimization_barrier(
        (exchange(weights, ("y", "x")), factor, total, kept, z)
    )
    partner = swapped(weights)
    pieces = total.reshape(line // cores, cores, rows, width)[z % (line // cores)]
    mine, other = (lax.dynamic_index_in_dim(pieces, i, 0, False) for i in (core, 1 - core))
    own_total = jnp.where(near, mine, swapped(other))
    whole = jax.ShapeDtypeStruct((planes, cores, held, width), jnp.bfloat16)
    own, scale = (rows, width), (1, rows)
    results = [(own, jnp.float32)] + [(own, jnp.bfloat16), (scale, jnp.float32)] * 2
    vmem, anywhere = (pl.BlockSpec(memory_space=space) for space in (pltpu.VMEM, pl.ANY))
    weights = pl.pallas_call(
        lay,
        out_shape=whole,
        in_specs=[vmem],
        out_specs=anywhere,
        scratch_shapes=[pltpu.SemaphoreType.DMA((PARTS,))],
        compiler_params=small,
    )(weights)
    weights, *results = pl.pallas_call(
        lay_and_advance,
        out_shape=[whole] + [jax.ShapeDtypeStruct(*result) for result in results],
        in_specs=[vmem] * 4 + [anywhere],
        out_specs=[anywhere] * 6,
        scratch_shapes=[pltpu.VMEM(*result) for result in results] + [pltpu.SemaphoreType.DMA((PARTS + 5,))],
        input_output_aliases={4: 0},
        compiler_params=small,
    )(partner, factor, own_total, kept, weights)
    master_new, first_q_new, first_scale_new, second_q_new, second_scale_new = results
    weights = weights.reshape(blocks, width)
    return (weights, master_new, first_q_new, first_scale_new[0], second_q_new, second_scale_new[0])


def solution(mesh):
    torus = Mesh(mesh.devices.reshape(4, 4, 8, 2), DP)
    in_specs = (P(DP, None, None), P(DP, None), P(DP, None), P(DP), P(DP, None), P(DP))
    out_specs = (P(), P(DP, None), P(DP, None), P(DP), P(DP, None), P(DP))
    return jax.shard_map(
        shards, mesh=torus, in_specs=in_specs, out_specs=out_specs, check_vma=False
    )
```

```python
import functools
import math

import jax
import jax.numpy as jnp
from jax import lax
from jax.experimental import pallas as pl
from jax.experimental.pallas import tpu as pltpu
from jax.sharding import Mesh
from jax.sharding import PartitionSpec as P

DP = ("y", "x", "z", "c")
PARTS = 4


beta_one = 0.9
beta_two = 0.95
learn_rate = 0.05
decay_rate = 0.1
adam_epsilon = 1e-08
clip_rms = 0.01
first_fix = 1.0 - 0.9**10
second_fix = 1.0 - 0.95**10


def exchange(x, axes):
    return lax.all_to_all(x, axes, split_axis=0, concat_axis=0, tiled=True)


def odd(z):
    return (z ^ z >> 1) & 1


def exchange_halves(x):
    y, x_, line, cores = (lax.axis_size(axis) for axis in DP)
    groups = [
        [(plane * line + z) * cores + (half ^ odd(z)) for plane in range(y * x_) for half in range(cores)]
        for z in range(line)
    ]
    return lax.all_to_all(x, DP, split_axis=0, concat_axis=0, tiled=True, axis_index_groups=groups)


def sent_to_all(x, axes):
    return exchange(jnp.broadcast_to(x, (lax.axis_size(axes), *x.shape)), axes)


def swapped(x):
    return lax.ppermute(x, "c", [(0, 1), (1, 0)])


def from_partner(x, flip):
    line = lax.axis_size("z")
    route = [(2 * z + c, 2 * (z ^ flip) + (c ^ odd(flip))) for z in range(line) for c in range(2)]
    return lax.ppermute(x, ("z", "c"), route)


def doubled(x, place, step):
    flip, level = step
    other = from_partner(x, flip)
    mine = jnp.arange(2) == (place[:, None] >> level & 1)
    place = jnp.where(mine, place[:, None], place[:, None] ^ flip).reshape(-1)
    x = jnp.where(mine.reshape(mine.shape + (1,) * (x.ndim - 1)), x[:, None], other[:, None])
    return x.reshape(-1, *x.shape[2:]), place


def advance(clipped, master, first, second):
    first_new = beta_one * first + (1.0 - beta_one) * clipped
    second_new = beta_two * second + (1.0 - beta_two) * clipped * clipped
    change = first_new / first_fix / (jnp.sqrt(second_new / second_fix) + adam_epsilon)
    master_new = master * (1.0 - learn_rate * decay_rate) - learn_rate * change
    return master_new, first_new, second_new


def clip_and_advance(limit, norms, total, states, weights, factors):
    pairs = norms[...]
    squares = jnp.sum(pairs[:, 0] + pairs[:, 1], keepdims=True)
    factor = jnp.minimum(1.0, limit / (jnp.sqrt(squares) + 1e-06))
    factors[...] = jnp.broadcast_to(factor, factors.shape)
    line, _, rows, width = states.shape
    for z in range(line):
        place = pl.ds(z * rows, rows)
        new, _, _ = advance(factor * total[place], states[z, 0], states[z, 1], states[z, 2])
        new = new.astype(weights.dtype)
        for plane in range(weights.shape[0]):
            weights[plane, place] = new


def copies_of_half(half, out, other, sent):
    side = lax.axis_index("c") ^ odd(lax.axis_index("z")) ^ other
    planes = half.shape[0] // PARTS
    spans = [pl.ds(part * planes, planes) for part in range(PARTS)]
    return [
        pltpu.make_async_copy(half.at[span], out.at[span, side], sent.at[part])
        for part, span in enumerate(spans)
    ]


def lay(half, out, sent):
    copies = copies_of_half(half, out, 0, sent)
    for copy in copies:
        copy.start()
    for copy in copies:
        copy.wait()


def lay_and_advance(half, factor, own, states, _, out, *refs):
    results, held, sent = refs[:5], refs[5:10], refs[10]
    copies = copies_of_half(half, out, 1, sent)
    for copy in copies:
        copy.start()

    rows = own.shape[0]
    held[0][...], *new = advance(factor[:1] * own[...], states[0], states[1], states[2])
    square = (rows, rows)
    diagonal = lax.broadcasted_iota(jnp.int32, square, 0) == lax.broadcasted_iota(jnp.int32, square, 1)
    for moment, quotient, scale in zip(new, held[1::2], held[2::2]):
        largest = jnp.max(jnp.abs(moment), axis=1, keepdims=True) + 1e-08
        quotient[...] = (moment / largest).astype(quotient.dtype)
        scale[...] = jnp.sum(jnp.where(diagonal, largest, 0.0), axis=0, keepdims=True)
    for i, (result, kept) in enumerate(zip(results, held)):
        copies.append(pltpu.make_async_copy(kept, result, sent.at[PARTS + i]))
        copies[-1].start()
    for copy in copies:
        copy.wait()


def shards(grads, master, first_q, first_scale, second_q, second_scale):
    blocks, width = grads.shape[1:]
    rows = master.shape[0]
    planes, line, cores = lax.axis_size(("y", "x")), lax.axis_size("z"), lax.axis_size("c")
    held = line * rows
    first = first_q.astype(jnp.float32) * first_scale[:, None]
    second = second_q.astype(jnp.float32) * second_scale[:, None]

    z, core = lax.axis_index("z"), lax.axis_index("c")
    near = z // (line // cores) == core ^ odd(z)
    chunks = line // cores * cores

    arrived = exchange_halves(grads[0].reshape(planes * cores, held, width))
    kept = jnp.stack([master, first, second])
    chip = jnp.where((jnp.arange(cores) == core)[:, None, None, None], kept, swapped(kept))
    states = jnp.where(near, chip, from_partner(chip, 6))[None]
    place = jnp.where(near, z, z ^ 6)[None]
    states, place = doubled(states, place, (2, 1))
    arrived, states = lax.optimization_barrier((arrived, states))
    part = arrived.astype(jnp.float32).sum(axis=0)

    total, states = lax.optimization_barrier((part, states))
    whole, _ = doubled(states, place, (1, 0))
    total = total + from_partner(total, 1)
    others = [from_partner(total, flip) for flip in (2, 6, 4)]
    others, states = lax.optimization_barrier((others, whole))
    total = (total + others[0]) + (others[1] + others[2])
    states = states.reshape(chunks, 3, rows, width)
    norms = sent_to_all(jnp.sum(total * total, axis=0, keepdims=True), ("y", "x", "c"))
    norms, total, states = lax.optimization_barrier((norms, total, states))
    small = pltpu.CompilerParams(vmem_limit_bytes=4 << 20)
    weights, factor = pl.pallas_call(
        functools.partial(clip_and_advance, clip_rms * math.sqrt(blocks * width)),
        out_shape=(
            jax.ShapeDtypeStruct((planes, held, width), jnp.bfloat16),
            jax.ShapeDtypeStruct((8, width), jnp.float32),
        ),
        compiler_params=small,
    )(norms.reshape(planes, cores, width), total, states)

    weights, factor, total, kept, z = lax.optimization_barrier(
        (exchange(weights, ("y", "x")), factor, total, kept, z)
    )
    partner = swapped(weights)
    pieces = total.reshape(line // cores, cores, rows, width)[z % (line // cores)]
    mine, other = (lax.dynamic_index_in_dim(pieces, i, 0, False) for i in (core, 1 - core))
    own_total = jnp.where(near, mine, swapped(other))
    whole = jax.ShapeDtypeStruct((planes, cores, held, width), jnp.bfloat16)
    own, scale = (rows, width), (1, rows)
    results = [(own, jnp.float32)] + [(own, jnp.bfloat16), (scale, jnp.float32)] * 2
    vmem, anywhere = (pl.BlockSpec(memory_space=space) for space in (pltpu.VMEM, pl.ANY))
    weights = pl.pallas_call(
        lay,
        out_shape=whole,
        in_specs=[vmem],
        out_specs=anywhere,
        scratch_shapes=[pltpu.SemaphoreType.DMA((PARTS,))],
        compiler_params=small,
    )(weights)
    weights, *results = pl.pallas_call(
        lay_and_advance,
        out_shape=[whole] + [jax.ShapeDtypeStruct(*result) for result in results],
        in_specs=[vmem] * 4 + [anywhere],
        out_specs=[anywhere] * 6,
        scratch_shapes=[pltpu.VMEM(*result) for result in results] + [pltpu.SemaphoreType.DMA((PARTS + 5,))],
        input_output_aliases={4: 0},
        compiler_params=small,
    )(partner, factor, own_total, kept, weights)
    master_new, first_q_new, first_scale_new, second_q_new, second_scale_new = results
    weights = weights.reshape(blocks, width)
    return (weights, master_new, first_q_new, first_scale_new[0], second_q_new, second_scale_new[0])


def solution(mesh):
    torus = Mesh(mesh.devices.reshape(4, 4, 8, 2), DP)
    in_specs = (P(DP, None, None), P(DP, None), P(DP, None), P(DP), P(DP, None), P(DP))
    out_specs = (P(), P(DP, None), P(DP, None), P(DP), P(DP, None), P(DP))
    return jax.shard_map(
        shards, mesh=torus, in_specs=in_specs, out_specs=out_specs, check_vma=False
    )
```
